32 devices in a mesh: gz: 8 (over y, x, core), xy: 4 (over z).
Axes of the slice: x: 2, y: 2, z: 4, core: 2. Of those that a mesh axis runs over, the one named last changes fastest.
Arguments:
- patches: bfloat16 [8, 8, 16, 128, 128], P('gz', 'xy'), may hold values from -6 to 6
- peak_offsets: int32 [8, 6, 8, 16], P('gz', None, 'xy'), may hold values from -4 to 4
- valid_masks: int32 [8, 3, 8, 16], P('gz', None, 'xy'), may hold values 0 or 1
- initial_positions: float32 [2, 8, 128, 256], P(None, 'gz', 'xy'), may hold values from -40 to 40
Outputs:
- positions: float32 [2, 8, 128, 256], P(None, 'gz', 'xy')
- targets: float32 [8, 6, 8, 16], P('gz', None, 'xy')
- surfaces: bfloat16 [8, 3, 8, 16, 128, 128], P('gz', None, 'xy')
- force_rms: float32 [4], replicated
The draws below stay inside these ranges and needn't reach their ends.
All inputs are finite; a program needn't handle non-finite values. No bound on the sum of `valid_masks` on one device may be relied on, other than what follows from the above.
Results may differ from the reference program's by a relative error of at most 0.0091.
Values may be sent and summed in bfloat16 or wider, within the bound.
A program may use at most 64 MiB of HBM per device.

```python
import math
import jax
import jax.numpy as jnp
from jax import lax

S = 128
SUB = 16
GC = 16
ITERS = 4
NZ = 8
GR = 8
NROWS = 128
NCOLS = 256


def draw_initial_positions(key, part):
    first_key = jax.random.fold_in(key, 0)
    third_key = jax.random.fold_in(key, 2)
    fourth_key = jax.random.fold_in(key, 3)
    depth_series = jnp.arange(NZ, dtype=jnp.float32)
    growth = 1.0 + 2.0 * depth_series / max(NZ - 1, 1)
    roughness = jax.random.uniform(third_key, (NZ,), jnp.float32, 0.75, 1.25)
    jitter = jax.random.uniform(fourth_key, (NROWS,), jnp.float32, 0.0, 1.0)
    level = (jnp.arange(NROWS, dtype=jnp.float32) + jitter) / NROWS
    base = jax.random.normal(first_key, (2, NZ, NROWS, NCOLS), jnp.float32)
    base = jnp.clip(base, -3.3, 3.3)
    row_scale = 0.3 * jnp.power(10.0, level)
    depth_scale = growth * roughness
    return base * depth_scale[None, :, None, None] * row_scale[None, None, :, None]


def plant(result, key, smallest, top_value):
    dims = result.shape
    spot = [jax.random.randint(jax.random.fold_in(key, axis), (), 0, dims[axis]) for axis in range(len(dims))]
    result = result.at[tuple(spot)].set(smallest)
    longest = dims.index(max(dims))
    spot[longest] = (spot[longest] + 1) % dims[longest]
    return result.at[tuple(spot)].set(top_value)


def steps_of(stream_key, shape, cuts, low, top_value):
    gain, own = 1.0, jax.random.fold_in(stream_key, 6)
    for position, blocks in cuts:
        steps = jnp.exp(jax.random.uniform(jax.random.fold_in(own, position), (blocks,), jnp.float32, low / len(cuts), top_value / len(cuts)))
        gain = gain * jnp.repeat(steps, shape[position] // blocks).reshape([-1 if axis == position else 1 for axis in range(len(shape))])
    return gain


def noise(key, extent, deviation, limit, pieces=(), held_as=jnp.bfloat16):
    values = deviation * jax.random.normal(key, extent, jnp.float32)
    if pieces:
        values = values * steps_of(key, extent, pieces, -0.22, 0.18)
    return jnp.clip(values, -limit, limit).astype(held_as)


def setup_inputs(seed: int = 0) -> dict:
    arg_keys = jax.random.split(jax.random.key(seed), 5)
    patches = noise(arg_keys[0], (NZ, GR, GC, S, S), 1.0, 6.0, ((0, 8), (1, 4)))
    peak_offsets = plant(jax.random.randint(arg_keys[1], (NZ, 6, GR, GC), -4, 5), jax.random.fold_in(arg_keys[1], 1), -4, 4).astype(jnp.int32)
    valid_masks = plant((jax.random.randint(arg_keys[2], (NZ, 3, GR, GC), 0, 4) < 3).astype(jnp.int32), jax.random.fold_in(arg_keys[2], 1), 0, 1)
    initial_positions = draw_initial_positions(jax.random.fold_in(arg_keys[4], 71), 0)
    return {"patches": patches, "peak_offsets": peak_offsets, "valid_masks": valid_masks, "initial_positions": initial_positions}


lattice_stiff = 0.5
clip_level = 5.0
step_size = 0.2
floor_ratio = 0.4
tiny_eps = 1e-06

def dft_tables(length):
    series = jnp.arange(length, dtype=jnp.int32)
    product = series[:, None] * series[None, :] % length
    angles = 2.0 * math.pi / length * product.astype(jnp.float32)
    return (jnp.cos(angles).astype(jnp.bfloat16), jnp.sin(angles).astype(jnp.bfloat16))

def rounded(value):
    return lax.optimization_barrier(value.astype(jnp.bfloat16)).astype(jnp.float32)

def spectrum(tiles, cosine, sine):
    row_cos = rounded(jnp.einsum('pab,bk->pak', tiles, cosine))
    row_sin = rounded(jnp.einsum('pab,bk->pak', tiles, sine))
    real = jnp.einsum('ja,pak->pjk', cosine, row_cos) - jnp.einsum('ja,pak->pjk', sine, row_sin)
    imag = -(jnp.einsum('ja,pak->pjk', sine, row_cos) + jnp.einsum('ja,pak->pjk', cosine, row_sin))
    return (real, imag)

def correlate(first, second, cosine, sine, length):
    cross_real = rounded(first[0] * second[0] + first[1] * second[1])
    cross_imag = rounded(first[0] * second[1] - first[1] * second[0])
    half_real = rounded(jnp.einsum('pab,bk->pak', cross_real, cosine) - jnp.einsum('pab,bk->pak', cross_imag, sine))
    half_imag = rounded(jnp.einsum('pab,bk->pak', cross_real, sine) + jnp.einsum('pab,bk->pak', cross_imag, cosine))
    whole = jnp.einsum('ja,pak->pjk', cosine, half_real) - jnp.einsum('ja,pak->pjk', sine, half_imag)
    return whole / float(length * length)

def refine(corr, shift_rows, shift_cols, length):
    series = jnp.arange(length, dtype=jnp.int32)
    taps = jnp.arange(3, dtype=jnp.int32) - 1
    row_index = (shift_rows[:, None] + taps[None, :] + length) % length
    col_index = (shift_cols[:, None] + taps[None, :] + length) % length
    row_pick = (series[None, None, :] == row_index[:, :, None]).astype(jnp.float32)
    col_pick = (series[None, None, :] == col_index[:, :, None]).astype(jnp.float32)
    partial_rows = jnp.einsum('pta,pab->ptb', row_pick, corr, precision=lax.Precision.HIGHEST)
    values = jnp.einsum('ptb,psb->pts', partial_rows, col_pick, precision=lax.Precision.HIGHEST)
    floor_value = floor_ratio * length
    along_rows = values[:, :, 1]
    along_cols = values[:, 1, :]
    sub_rows = (along_rows[:, 2] - along_rows[:, 0]) / jnp.maximum(lax.optimization_barrier(jnp.sum(jnp.abs(along_rows), axis=1)), floor_value)
    sub_cols = (along_cols[:, 2] - along_cols[:, 0]) / jnp.maximum(lax.optimization_barrier(jnp.sum(jnp.abs(along_cols), axis=1)), floor_value)
    return (shift_rows.astype(jnp.float32) + sub_rows, shift_cols.astype(jnp.float32) + sub_cols)

def raise_depth(array, distance, axis):
    zeros = jnp.zeros_like(lax.slice_in_dim(array, 0, distance, axis=axis))
    joined = jnp.concatenate([array, zeros], axis=axis)
    return lax.slice_in_dim(joined, distance, distance + array.shape[axis], axis=axis)

def lower_depth(array, distance, axis):
    zeros = jnp.zeros_like(lax.slice_in_dim(array, 0, distance, axis=axis))
    joined = jnp.concatenate([zeros, array], axis=axis)
    return lax.slice_in_dim(joined, 0, array.shape[axis], axis=axis)

def expand_nodes(array, axis):
    return jnp.repeat(jnp.repeat(array, SUB, axis=axis), SUB, axis=axis + 1)

def reference(patches, peak_offsets, valid_masks, initial_positions):
    tiles_count = GR * GC
    cos_table, sin_table = dft_tables(S)
    cosine = cos_table.astype(jnp.float32)
    sine = sin_table.astype(jnp.float32)
    padded = jnp.concatenate([patches, jnp.zeros((3, GR, GC, S, S), jnp.bfloat16)], axis=0)

    def one_section(depth_index):
        window = lax.dynamic_slice_in_dim(padded, depth_index, 4, 0).astype(jnp.float32).reshape(4, tiles_count, S, S)
        own = spectrum(window[0], cosine, sine)
        offsets = lax.dynamic_index_in_dim(peak_offsets, depth_index, 0, keepdims=False).reshape(6, tiles_count)
        results = []
        maps = []
        for distance in range(3):
            other = spectrum(window[distance + 1], cosine, sine)
            corr = correlate(own, other, cosine, sine, S)
            maps.append(corr.astype(jnp.bfloat16).reshape(GR, GC, S, S))
            rows_target, cols_target = refine(corr, offsets[2 * distance], offsets[2 * distance + 1], S)
            results.append(rows_target)
            results.append(cols_target)
        return (jnp.stack(results).reshape(6, GR, GC), jnp.stack(maps))
    targets, surfaces = lax.map(one_section, jnp.arange(NZ, dtype=jnp.int32))
    depth_series = jnp.arange(NZ, dtype=jnp.int32)
    weights = []
    vectors = []
    for distance in range(1, 4):
        live = (depth_series + distance < NZ).astype(jnp.float32)
        patch_weight = valid_masks[:, distance - 1].astype(jnp.float32) * (1.0 / distance) * live[:, None, None]
        weights.append(expand_nodes(patch_weight, 1))
        patch_vector = jnp.stack([targets[:, 2 * distance - 2], targets[:, 2 * distance - 1]], axis=0)
        vectors.append(expand_nodes(patch_vector, 2))
    count = 2.0 * NZ * NROWS * NCOLS
    positions = initial_positions
    norms = []
    for iteration in range(ITERS):
        edged = jnp.pad(positions, ((0, 0), (0, 0), (1, 1), (1, 1)), mode='edge')
        lattice = edged[:, :, :-2, 1:-1] + edged[:, :, 2:, 1:-1] + edged[:, :, 1:-1, :-2] + edged[:, :, 1:-1, 2:] - 4.0 * positions
        force = lattice_stiff * lattice
        for distance in range(1, 4):
            weight = weights[distance - 1]
            vector = vectors[distance - 1]
            above = raise_depth(positions, distance, 1)
            below = lower_depth(positions, distance, 1)
            weight_low = lower_depth(weight, distance, 0)
            vector_low = lower_depth(vector, distance, 1)
            force = force + weight * (above - positions - vector) - weight_low * (positions - below - vector_low)
        rms = jnp.sqrt(jnp.sum(force * force) / count + tiny_eps)
        factor = jnp.minimum(1.0, clip_level / rms)
        positions = positions + step_size * factor * force
        norms.append(rms)
    return (positions, targets, surfaces, jnp.stack(norms))
```

```python
import functools

import jax
import jax.numpy as jnp
import numpy as np
from jax import lax
from jax.experimental import pallas as pl
from jax.experimental.pallas import tpu as pltpu
from jax.sharding import PartitionSpec as P

SUB = 16
ITERS = 4
REACH = 3
GHOST = 8
GROUP = 4

lattice_stiff = 0.5
clip_level = 5.0
step_size = 0.2
floor_ratio = 0.4
tiny_eps = 1e-06

MESH = pl.DeviceIdType.MESH
F32 = jnp.float32
BF16 = jnp.bfloat16


def tables(length):
    series = np.arange(length, dtype=np.int64)
    product = (series[:, None] * series[None, :]) % length
    angles = np.float32(2.0 * np.pi / length) * product.astype(np.float32)
    cosine = np.cos(angles).astype(np.float32)
    sine = np.sin(angles).astype(np.float32)
    rows = np.concatenate([cosine, sine], axis=1)
    forward = np.block([[cosine, -sine], [-sine, -cosine]])
    back = np.block([[cosine, sine], [-sine, cosine]])
    last = np.concatenate([cosine, -sine], axis=1)
    return [jnp.asarray(t.astype(jnp.bfloat16)) for t in (rows, forward, back, last)]


def dot(left, right):
    return jnp.dot(left, right, preferred_element_type=F32)


def kernel(
    nz, nx, rows_dev, columns,
    patches, offsets, w_scale, w_rows, nodes, node_edges, own_nodes, t_rows, t_forward, t_back, t_last,
    surfaces, targets_out, positions_out, rms_out,
    arrived, spec_re, spec_im, staged, taps, met, sent_msg, gathered, all_nodes, ghosts,
    vec, weight, grams, mine,
    p_send, p_recv, n_send, n_recv, t_send, t_recv, g_send, g_recv, o_sem,
):
    z = lax.axis_index("gz")
    x = lax.axis_index("xy")
    length = patches.shape[-1]
    tiles = patches.shape[0]
    chunks = tiles // GROUP
    half_rows = nodes.shape[0] // 2
    high = half_rows + 2 * GHOST
    wide = nodes.shape[1]

    barrier = pltpu.get_barrier_semaphore()

    @pl.loop(0, nz)
    def _(zz):
        for xx in range(nx):
            @pl.when(jnp.logical_or(zz != z, x != xx))
            def _():
                pl.semaphore_signal(barrier, inc=1, device_id=(zz, xx), device_id_type=MESH)

    pl.semaphore_wait(barrier, nz * nx - 1)

    def chunk_ref(ref, c):
        return ref.at[pl.ds(c * GROUP, GROUP)]

    def patch_copy(d, c):
        source = chunk_ref(patches, c) if d == 0 else chunk_ref(arrived.at[d - 1], c)
        return pltpu.make_async_remote_copy(
            src_ref=source,
            dst_ref=chunk_ref(arrived.at[d], c),
            send_sem=p_send.at[d, c],
            recv_sem=p_recv.at[d, c],
            device_id=(jnp.maximum(z - 1, 0), x),
            device_id_type=MESH,
        )

    @pl.when(z > 0)
    def _():
        @pl.loop(0, chunks)
        def _(c):
            patch_copy(0, c).start()

    def fan(sources, targets, send, recv, act):
        @pl.loop(0, nz)
        def _(zz):
            for slot, test, xx in (
                (1, zz != z, x),
                (0, x + 1 < nx, jnp.minimum(x + 1, nx - 1)),
                (2, x > 0, jnp.maximum(x - 1, 0)),
            ):
                @pl.when(test)
                def _():
                    copy = pltpu.make_async_remote_copy(
                        src_ref=sources[slot],
                        dst_ref=targets[slot].at[z],
                        send_sem=send.at[slot, zz],
                        recv_sem=recv.at[slot, z],
                        device_id=(zz, xx),
                        device_id_type=MESH,
                    )
                    if act == "start":
                        copy.start()
                    else:
                        copy.wait_send()

    def fan_wait(sources, targets, send, recv):
        @pl.loop(0, nz)
        def _(zz):
            for slot, test, xx in ((1, zz != z, x), (0, x > 0, x), (2, x + 1 < nx, x)):
                @pl.when(test)
                def _():
                    pltpu.make_async_remote_copy(
                        src_ref=sources[slot],
                        dst_ref=targets[slot].at[zz],
                        send_sem=send.at[slot, zz],
                        recv_sem=recv.at[slot, zz],
                        device_id=(zz, xx),
                        device_id_type=MESH,
                    ).wait_recv()

    node_from = (node_edges.at[1], nodes, node_edges.at[0])
    node_to = (ghosts.at[0], all_nodes, ghosts.at[1])
    fan(node_from, node_to, n_send, n_recv, "start")

    def spectra(block):
        lines = dot(block.reshape(GROUP * length, length), t_rows[...]).astype(BF16)
        found = []
        for t in range(GROUP):
            one = lines[t * length : (t + 1) * length]
            pair = jnp.concatenate([one[:, :length], one[:, length:]], axis=0)
            both = dot(t_forward[...], pair)
            found.append((both[:length], both[length:]))
        return found

    @pl.loop(0, chunks)
    def _(c):
        for t, (real, imag) in enumerate(spectra(patches[pl.ds(c * GROUP, GROUP)])):
            spec_re[c * GROUP + t] = real
            spec_im[c * GROUP + t] = imag

    row_at = lax.broadcasted_iota(jnp.int32, (16, length), 0)
    row_at = jnp.where(row_at < 8, row_at, row_at - 16)
    col_at = lax.broadcasted_iota(jnp.int32, (1, length), 1)
    col_at = jnp.where(col_at < length // 2, col_at, col_at - length)

    for d in range(1, REACH + 1):
        live = z + d < nz

        @pl.when(jnp.logical_not(live))
        def _():
            arrived[d - 1] = jnp.zeros(arrived.shape[1:], arrived.dtype)

        @pl.loop(0, chunks)
        def _(c):
            @pl.when(live)
            def _():
                patch_copy(d - 1, c).wait_recv()

            if d < REACH:
                @pl.when(jnp.logical_and(live, z > 0))
                def _():
                    patch_copy(d, c).start()

            cross = []
            for t, (real, imag) in enumerate(spectra(arrived[d - 1, pl.ds(c * GROUP, GROUP)])):
                own_re = spec_re[c * GROUP + t]
                own_im = spec_im[c * GROUP + t]
                cross_re = (own_re * real + own_im * imag).astype(BF16)
                cross_im = (own_re * imag - own_im * real).astype(BF16)
                cross.append(jnp.concatenate([cross_re, cross_im], axis=1))
            half = dot(jnp.concatenate(cross, axis=0), t_back[...]).astype(BF16)
            for t in range(GROUP):
                tile = c * GROUP + t
                one = half[t * length : (t + 1) * length]
                pair = jnp.concatenate([one[:, :length], one[:, length:]], axis=0)
                corr = dot(t_last[...], pair) * (1.0 / float(length * length))
                staged[d - 1, tile] = corr.astype(BF16)
                near = jnp.concatenate([corr[:8], corr[length - 8 :]], axis=0)
                shift_row = offsets[2 * d - 2, pl.ds(tile, 1)]
                shift_col = offsets[2 * d - 1, pl.ds(tile, 1)]
                lines = [
                    jnp.sum(jnp.where(row_at == shift_row + s, near, 0.0), axis=0, keepdims=True)
                    for s in (-1, 0, 1)
                ]
                here = col_at == shift_col
                for s in range(3):
                    taps[s, d - 1, pl.ds(tile, 1)] = jnp.where(here, lines[s], 0.0)
                taps[3, d - 1, pl.ds(tile, 1)] = jnp.where(col_at == shift_col - 1, lines[1], 0.0)
                taps[4, d - 1, pl.ds(tile, 1)] = jnp.where(col_at == shift_col + 1, lines[1], 0.0)
            pltpu.make_async_copy(
                chunk_ref(staged.at[d - 1], c), chunk_ref(surfaces.at[d - 1], c), o_sem.at[d - 1, c]
            ).start()

    lane_tile = lax.broadcasted_iota(jnp.int32, (tiles, 128), 1)
    row_tile = lax.broadcasted_iota(jnp.int32, (tiles, 128), 0)
    level = floor_ratio * length
    lines = []
    for d in range(REACH):
        value = [jnp.sum(taps[s, d], axis=1, keepdims=True) for s in range(5)]
        for axis, (low, mid, top) in enumerate(((0, 1, 2), (3, 1, 4))):
            low, mid, top = value[low], value[mid], value[top]
            size = jnp.maximum(jnp.abs(low) + jnp.abs(mid) + jnp.abs(top), level)
            found = offsets[2 * d + axis].astype(F32) + (top - low) / size
            lines.append(
                jnp.sum(jnp.where(lane_tile == row_tile, found, 0.0), axis=0, keepdims=True)
            )
    message = jnp.concatenate(lines + [jnp.zeros((8 - 2 * REACH, 128), F32)], axis=0)
    targets_out[...] = message
    message = message * w_scale[...] + w_rows[...]
    sent_msg[...] = message
    gathered[1, z] = message
    message_from = (sent_msg, sent_msg, sent_msg)
    message_to = (gathered.at[0], gathered.at[1], gathered.at[2])
    fan(message_from, message_to, t_send, t_recv, "start")

    fan_wait(node_from, node_to, n_send, n_recv)
    all_nodes[z] = nodes[...]

    @pl.when(x == 0)
    def _():
        ghosts[0] = jnp.zeros(ghosts.shape[1:], ghosts.dtype)
        gathered[0] = jnp.zeros(gathered.shape[1:], gathered.dtype)

    @pl.when(x == nx - 1)
    def _():
        ghosts[1] = jnp.zeros(ghosts.shape[1:], ghosts.dtype)
        gathered[2] = jnp.zeros(gathered.shape[1:], gathered.dtype)

    for i in range(ITERS):
        for part in range(2):
            for pad in range(REACH):
                vec[i, part, pad] = jnp.zeros((high, wide), F32)
                vec[i, part, nz + REACH + pad] = jnp.zeros((high, wide), F32)
    for k in range(REACH):
        for pad in range(REACH):
            weight[k, pad] = jnp.zeros((high, wide), F32)

    @pl.loop(0, nz)
    def _(zz):
        body = all_nodes[zz].astype(F32)
        above = ghosts[0, zz].astype(F32)
        below = ghosts[1, zz].astype(F32)
        for part in range(2):
            vec[0, part, zz + REACH, pl.ds(0, GHOST)] = above[part * GHOST : (part + 1) * GHOST]
            vec[0, part, zz + REACH, pl.ds(GHOST, half_rows)] = body[
                part * half_rows : (part + 1) * half_rows
            ]
            vec[0, part, zz + REACH, pl.ds(GHOST + half_rows, GHOST)] = below[
                part * GHOST : (part + 1) * GHOST
            ]

    fan_wait(message_from, message_to, t_send, t_recv)

    pick_from = lax.broadcasted_iota(jnp.int32, (128, wide), 0)
    pick_to = lax.broadcasted_iota(jnp.int32, (128, wide), 1) // SUB

    def spread(slot, line, base):
        pick = (pick_from == pick_to + (base + line * columns)).astype(F32)
        return jnp.dot(
            gathered[slot].reshape(nz * 8, 128), pick,
            precision=lax.Precision.HIGHEST, preferred_element_type=F32,
        )

    pieces = (
        [(0, rows_dev - 1, 0, GHOST)]
        + [(1, r, GHOST + r * SUB, SUB) for r in range(rows_dev)]
        + [(2, 0, GHOST + half_rows, GHOST)]
    )
    for slot, line, start, count in pieces:
        met[0] = spread(slot, line, 0)
        met[1] = spread(slot, line, rows_dev * columns)

        @pl.loop(0, nz)
        def _(zz):
            for k in range(REACH):
                weight[k, zz + REACH, pl.ds(start, count)] = jnp.broadcast_to(
                    met[1, pl.ds(zz * 8 + k, 1)], (count, wide)
                )
            for part in range(2):
                total = jnp.zeros((1, wide), F32)
                for k in range(REACH):
                    here = met[0, pl.ds(zz * 8 + 2 * k + part, 1)]
                    behind = jnp.maximum(zz - k - 1, 0)
                    back = met[0, pl.ds(behind * 8 + 2 * k + part, 1)]
                    total = total - here + jnp.where(zz > k, back, 0.0)
                vec[ITERS, part, zz + REACH, pl.ds(start, count)] = jnp.broadcast_to(
                    total, (count, wide)
                )

    row_id = lax.broadcasted_iota(jnp.int32, (high, wide), 0)
    col_id = lax.broadcasted_iota(jnp.int32, (high, wide), 1)
    first = jnp.logical_and(row_id == GHOST, x == 0)
    final = jnp.logical_and(row_id == GHOST + half_rows - 1, x == nx - 1)

    def apply(source, target, extra):
        @pl.loop(0, nz)
        def _(zz):
            at = zz + REACH
            for part in range(2):
                v = vec[source, part, at]
                up = jnp.where(first, v, pltpu.roll(v, 1, 0))
                down = jnp.where(final, v, pltpu.roll(v, high - 1, 0))
                left = jnp.where(col_id == 0, v, pltpu.roll(v, 1, 1))
                right = jnp.where(col_id == wide - 1, v, pltpu.roll(v, wide - 1, 1))
                force = lattice_stiff * (up + down + left + right - 4.0 * v)
                if extra is not None:
                    force = force + vec[extra, part, at]
                for k in range(1, REACH + 1):
                    force = force + weight[k - 1, at] * (vec[source, part, at + k] - v)
                    force = force - weight[k - 1, at - k] * (v - vec[source, part, at - k])
                vec[target, part, at] = force

    apply(0, 1, ITERS)
    for i in range(1, ITERS):
        apply(i, i + 1, None)

    pairs = [(i, j) for i in range(ITERS) for j in range(i, ITERS)]

    def products(zz, held):
        held = list(held)
        for part in range(2):
            values = [
                vec[i + 1, part, zz + REACH, pl.ds(GHOST, half_rows)].reshape(
                    half_rows // 8, 8, wide
                )
                for i in range(ITERS)
            ]
            for n, (i, j) in enumerate(pairs):
                held[n] = held[n] + jnp.sum(values[i] * values[j], axis=0)
        return tuple(held)

    held = lax.fori_loop(0, nz, products, tuple(jnp.zeros((8, wide), F32) for _ in pairs))
    lane = lax.broadcasted_iota(jnp.int32, (8, 128), 1)
    gram = jnp.zeros((8, 128), F32)
    for n in range(len(pairs)):
        line = jnp.sum(held[n], axis=0, keepdims=True)
        gram = jnp.where(lane == n, jnp.sum(line, axis=1, keepdims=True), gram)
    mine[...] = gram
    grams[x] = gram

    def gram_copy(xx, where):
        return pltpu.make_async_remote_copy(
            src_ref=mine,
            dst_ref=grams.at[where],
            send_sem=g_send.at[xx],
            recv_sem=g_recv.at[where],
            device_id=(z, xx),
            device_id_type=MESH,
        )

    for xx in range(nx):
        @pl.when(xx != x)
        def _():
            gram_copy(xx, x).start()
    for xx in range(nx):
        @pl.when(xx != x)
        def _():
            gram_copy(xx, xx).wait_recv()
    total = grams[0]
    for xx in range(1, nx):
        total = total + grams[xx]
    total = total[:1]
    lane = lax.broadcasted_iota(jnp.int32, (1, 128), 1)
    inner = {}
    for n, (i, j) in enumerate(pairs):
        inner[i, j] = jnp.sum(jnp.where(lane == n, total, 0.0), axis=1, keepdims=True)
        inner[j, i] = inner[i, j]
    count = 2.0 * nz * nx * half_rows * wide
    factors = [jnp.ones((1, 1), F32)]
    moved = [jnp.zeros((1, 1), F32) for _ in range(ITERS)]
    report = jnp.zeros((1, 128), F32)
    for i in range(ITERS):
        size = jnp.zeros((1, 1), F32)
        for a in range(i + 1):
            for b in range(i + 1):
                size = size + factors[a] * factors[b] * inner[a, b]
        rms = jnp.sqrt(jnp.maximum(size, 0.0) / count + tiny_eps)
        report = jnp.where(lane == i, rms, report)
        step = step_size * jnp.minimum(1.0, clip_level / rms)
        for a in range(i + 1):
            moved[a] = moved[a] + step * factors[a]
        later = factors + [jnp.zeros((1, 1), F32)]
        for a in range(i + 1):
            later[a + 1] = later[a + 1] + step * factors[a]
        factors = later
    rms_out[...] = report
    for part in range(2):
        result = own_nodes[part]
        for i in range(ITERS):
            result = result + moved[i] * vec[i + 1, part, z + REACH, pl.ds(GHOST, half_rows)]
        positions_out[part] = result

    for xx in range(nx):
        @pl.when(xx != x)
        def _():
            gram_copy(xx, x).wait_send()
    fan(node_from, node_to, n_send, n_recv, "wait")
    fan(message_from, message_to, t_send, t_recv, "wait")
    for d in range(REACH):
        @pl.when(jnp.logical_and(z > 0, z + d < nz))
        def _():
            @pl.loop(0, chunks)
            def _(c):
                patch_copy(d, c).wait_send()

        @pl.loop(0, chunks)
        def _(c):
            pltpu.make_async_copy(
                chunk_ref(staged.at[d], c), chunk_ref(surfaces.at[d], c), o_sem.at[d, c]
            ).wait()


def local(nz, nx, patches, peak_offsets, valid_masks, initial_positions):
    length = patches.shape[-1]
    rows_dev, columns = patches.shape[1:3]
    tiles = rows_dev * columns
    chunks = tiles // GROUP
    half_rows, wide = initial_positions.shape[2:]
    high = half_rows + 2 * GHOST
    z = lax.axis_index("gz")
    offsets = jnp.broadcast_to(peak_offsets.reshape(2 * REACH, tiles, 1), (2 * REACH, tiles, 128))
    reach = jnp.arange(1, REACH + 1)
    live = jnp.where(z + reach < nz, 1.0 / reach.astype(F32), 0.0)
    weights = valid_masks.reshape(REACH, tiles).astype(F32) * live[:, None]
    scale = jnp.pad(jnp.repeat(weights, 2, axis=0), ((0, 8 - 2 * REACH), (0, 128 - tiles)))
    lines = jnp.pad(weights, ((0, 8 - REACH), (tiles, 128 - 2 * tiles)))
    own = initial_positions[:, 0]
    narrow = own.astype(BF16)
    edges = jnp.stack([narrow[:, :GHOST], narrow[:, -GHOST:]]).reshape(2, 2 * GHOST, wide)
    vmem = pl.BlockSpec(memory_space=pltpu.VMEM)
    surfaces, targets, positions, rms = pl.pallas_call(
        functools.partial(kernel, nz, nx, rows_dev, columns),
        out_shape=(
            jax.ShapeDtypeStruct((REACH, tiles, length, length), BF16),
            jax.ShapeDtypeStruct((8, 128), F32),
            jax.ShapeDtypeStruct((2, half_rows, wide), F32),
            jax.ShapeDtypeStruct((1, 128), F32),
        ),
        in_specs=[vmem] * 11,
        out_specs=(pl.BlockSpec(memory_space=pl.ANY), vmem, vmem, vmem),
        scratch_shapes=[
            pltpu.VMEM((REACH, tiles, length, length), BF16),
            pltpu.VMEM((tiles, length, length), F32),
            pltpu.VMEM((tiles, length, length), F32),
            pltpu.VMEM((REACH, tiles, length, length), BF16),
            pltpu.VMEM((5, REACH, tiles, 128), F32),
            pltpu.VMEM((2, nz * 8, wide), F32),
            pltpu.VMEM((8, 128), F32),
            pltpu.VMEM((3, nz, 8, 128), F32),
            pltpu.VMEM((nz, 2 * half_rows, wide), BF16),
            pltpu.VMEM((2, nz, 2 * GHOST, wide), BF16),
            pltpu.VMEM((ITERS + 1, 2, nz + 2 * REACH, high, wide), F32),
            pltpu.VMEM((REACH, nz + REACH, high, wide), F32),
            pltpu.VMEM((nx, 8, 128), F32),
            pltpu.VMEM((8, 128), F32),
            pltpu.SemaphoreType.DMA((REACH, chunks)),
            pltpu.SemaphoreType.DMA((REACH, chunks)),
            pltpu.SemaphoreType.DMA((3, nz)),
            pltpu.SemaphoreType.DMA((3, nz)),
            pltpu.SemaphoreType.DMA((3, nz)),
            pltpu.SemaphoreType.DMA((3, nz)),
            pltpu.SemaphoreType.DMA((nx,)),
            pltpu.SemaphoreType.DMA((nx,)),
            pltpu.SemaphoreType.DMA((REACH, chunks)),
        ],
        compiler_params=pltpu.CompilerParams(
            collective_id=0, has_side_effects=True, vmem_limit_bytes=67043328
        ),
        name="align",
    )(
        patches.reshape(tiles, length, length), offsets, scale, lines,
        narrow.reshape(2 * half_rows, wide), edges, own, *tables(length),
    )
    return (
        positions[:, None],
        targets[: 2 * REACH, :tiles].reshape(1, 2 * REACH, rows_dev, columns),
        surfaces.reshape(1, REACH, rows_dev, columns, length, length),
        rms[0, :ITERS],
    )


def solution(mesh):
    in_specs = (
        P("gz", "xy", None, None, None),
        P("gz", None, "xy", None),
        P("gz", None, "xy", None),
        P(None, "gz", "xy", None),
    )
    out_specs = (
        P(None, "gz", "xy", None),
        P("gz", None, "xy", None),
        P("gz", None, "xy", None, None, None),
        P(),
    )
    body = functools.partial(local, mesh.shape["gz"], mesh.shape["xy"])
    return jax.shard_map(body, mesh=mesh, in_specs=in_specs, out_specs=out_specs, check_vma=False)
```

```python
import functools

import jax
import jax.numpy as jnp
import numpy as np
from jax import lax
from jax.experimental import pallas as pl
from jax.experimental.pallas import tpu as pltpu
from jax.sharding import PartitionSpec as P

SUB = 16
ITERS = 4
REACH = 3
GHOST = 8
GROUP = 4

lattice_stiff = 0.5
clip_level = 5.0
step_size = 0.2
floor_ratio = 0.4
tiny_eps = 1e-06

MESH = pl.DeviceIdType.MESH
F32 = jnp.float32
BF16 = jnp.bfloat16


def tables(length):
    series = np.arange(length, dtype=np.int64)
    product = (series[:, None] * series[None, :]) % length
    angles = np.float32(2.0 * np.pi / length) * product.astype(np.float32)
    cosine = np.cos(angles).astype(np.float32)
    sine = np.sin(angles).astype(np.float32)
    rows = np.concatenate([cosine, sine], axis=1)
    forward = np.block([[cosine, -sine], [-sine, -cosine]])
    back = np.block([[cosine, sine], [-sine, cosine]])
    last = np.concatenate([cosine, -sine], axis=1)
    return [jnp.asarray(t.astype(jnp.bfloat16)) for t in (rows, forward, back, last)]


def dot(left, right):
    return jnp.dot(left, right, preferred_element_type=F32)


def kernel(
    nz, nx, rows_dev, columns,
    patches, peaks, masks, own_nodes, t_rows, t_forward, t_back, t_last,
    surfaces, targets_out, positions_out, rms_out,
    arrived, spec_re, spec_im, offsets, trust, nodes, node_edges, taps, met, sent_msg, gathered, all_nodes, ghosts,
    vec, weight, grams, mine,
    p_send, p_recv, n_send, n_recv, t_send, t_recv, g_send, g_recv,
):
    z = lax.axis_index("gz")
    x = lax.axis_index("xy")
    length = patches.shape[-1]
    tiles = patches.shape[0]
    chunks = tiles // GROUP
    half_rows = nodes.shape[0] // 2
    high = half_rows + 2 * GHOST
    wide = nodes.shape[1]

    barrier = pltpu.get_barrier_semaphore()

    @pl.loop(0, nz)
    def _(zz):
        for xx in range(nx):
            @pl.when(jnp.logical_or(zz != z, x != xx))
            def _():
                pl.semaphore_signal(barrier, inc=1, device_id=(zz, xx), device_id_type=MESH)

    narrow = own_nodes[...].astype(BF16)
    for part in range(2):
        base = part * half_rows
        nodes[pl.ds(base, half_rows)] = narrow[part]
    node_edges[0] = jnp.concatenate([narrow[part, :GHOST] for part in range(2)], axis=0)
    node_edges[1] = jnp.concatenate([narrow[part, half_rows - GHOST :] for part in range(2)], axis=0)
    across = lax.broadcasted_iota(jnp.int32, (columns, columns), 1)
    along = lax.broadcasted_iota(jnp.int32, (columns, columns), 0)

    def upright(line):
        return jnp.sum(jnp.where(across == along, line, 0), axis=1, keepdims=True)

    for r in range(rows_dev):
        here = pl.ds(r * columns, columns)
        for q in range(2 * REACH):
            offsets[q, here] = jnp.broadcast_to(upright(peaks[q, r : r + 1, :]), (columns, 128))
        for k in range(REACH):
            share = jnp.where(z + k + 1 < nz, 1.0 / (k + 1), 0.0)
            trust[k, here] = jnp.broadcast_to(
                upright(masks[k, r : r + 1, :]).astype(F32) * share, (columns, 128)
            )

    for i in range(ITERS):
        for part in range(2):
            for pad in range(REACH):
                vec[i, part, pad] = jnp.zeros((high, wide), F32)
                vec[i, part, nz + REACH + pad] = jnp.zeros((high, wide), F32)
    for k in range(REACH):
        for pad in range(REACH):
            weight[k, pad] = jnp.zeros((high, wide), F32)

    pl.semaphore_wait(barrier, nz * nx - 1)

    def chunk_ref(ref, c):
        return ref.at[pl.ds(c * GROUP, GROUP)]

    def own_copy(kind, c):
        slot = 2 * kind
        return pltpu.make_async_remote_copy(
            src_ref=chunk_ref(patches, c),
            dst_ref=chunk_ref(arrived.at[slot], c),
            send_sem=p_send.at[kind, c],
            recv_sem=p_recv.at[slot, c],
            device_id=(z - 1 - slot, x),
            device_id_type=MESH,
        )

    def passed_copy(slot, c):
        later = (slot + 1) % 3
        return pltpu.make_async_remote_copy(
            src_ref=chunk_ref(arrived.at[slot], c),
            dst_ref=chunk_ref(arrived.at[later], c),
            send_sem=p_send.at[slot + 2, c],
            recv_sem=p_recv.at[later, c],
            device_id=(z - 1 + 3 * ((slot + 1) // 3), x),
            device_id_type=MESH,
        )

    own_tests = (z % 4 != 0, jnp.logical_and(z % 2 == 0, z >= 4))

    def passes(slot):
        one = jnp.logical_and(slot == 0, z > 0)
        two = jnp.logical_and(slot == 1, z % 2 == 1)
        three = jnp.logical_and(slot == 2, jnp.logical_and(z % 4 == 1, z + 2 < nz))
        return jnp.logical_and(jnp.logical_or(one, jnp.logical_or(two, three)), z + slot + 1 < nz)

    @pl.loop(0, chunks)
    def _(c):
        for kind in range(2):
            @pl.when(own_tests[kind])
            def _():
                own_copy(kind, c).start()

    def fan(sources, targets, send, recv, act):
        @pl.loop(0, nz)
        def _(zz):
            for slot, test, xx in (
                (1, zz != z, x),
                (0, x + 1 < nx, jnp.minimum(x + 1, nx - 1)),
                (2, x > 0, jnp.maximum(x - 1, 0)),
            ):
                @pl.when(test)
                def _():
                    copy = pltpu.make_async_remote_copy(
                        src_ref=sources[slot],
                        dst_ref=targets[slot].at[z],
                        send_sem=send.at[slot, zz],
                        recv_sem=recv.at[slot, z],
                        device_id=(zz, xx),
                        device_id_type=MESH,
                    )
                    if act == "start":
                        copy.start()
                    else:
                        copy.wait_send()

    def fan_wait(sources, targets, send, recv):
        @pl.loop(0, nz)
        def _(zz):
            for slot, test, xx in ((1, zz != z, x), (0, x > 0, x), (2, x + 1 < nx, x)):
                @pl.when(test)
                def _():
                    pltpu.make_async_remote_copy(
                        src_ref=sources[slot],
                        dst_ref=targets[slot].at[zz],
                        send_sem=send.at[slot, zz],
                        recv_sem=recv.at[slot, zz],
                        device_id=(zz, xx),
                        device_id_type=MESH,
                    ).wait_recv()

    node_from = (node_edges.at[1], nodes, node_edges.at[0])
    node_to = (ghosts.at[0], all_nodes, ghosts.at[1])
    fan(node_from, node_to, n_send, n_recv, "start")

    def spectra(block):
        lines = dot(block.reshape(GROUP * length, length), t_rows[...]).astype(BF16)
        found = []
        for t in range(GROUP):
            one = lines[t * length : (t + 1) * length]
            pair = jnp.concatenate([one[:, :length], one[:, length:]], axis=0)
            both = dot(t_forward[...], pair)
            found.append((both[:length], both[length:]))
        return found

    @pl.loop(0, chunks)
    def _(c):
        for t, (real, imag) in enumerate(spectra(patches[pl.ds(c * GROUP, GROUP)])):
            spec_re[c * GROUP + t] = real
            spec_im[c * GROUP + t] = imag

    row_at = lax.broadcasted_iota(jnp.int32, (16, length), 0)
    row_at = jnp.where(row_at < 8, row_at, row_at - 16)
    col_at = lax.broadcasted_iota(jnp.int32, (1, length), 1)
    col_at = jnp.where(col_at < length // 2, col_at, col_at - length)

    for slot in range(REACH):
        @pl.when(z + slot + 1 >= nz)
        def _():
            arrived[slot] = jnp.zeros(arrived.shape[1:], arrived.dtype)

    even = 1 - z % 2
    three = (z % 2) * ((z % 4) // 2)
    one = 1 - even - three

    @pl.loop(0, REACH * chunks)
    def _(n):
        ended = n // (2 * chunks)
        slot = (
            even * (n // chunks)
            + one * ((1 - ended) * (n % 2) * 2 + ended)
            + three * (n % 3)
        )
        c = (
            even * (n % chunks)
            + one * ((1 - ended) * (n // 2) + ended * (n - 2 * chunks))
            + three * (n // 3)
        )

        @pl.when(z + slot + 1 < nz)
        def _():
            passed_copy((slot + 2) % 3, c).wait_recv()

        @pl.when(passes(slot))
        def _():
            passed_copy(slot, c).start()

        cross = []
        for t, (real, imag) in enumerate(spectra(arrived[slot, pl.ds(c * GROUP, GROUP)])):
            own_re = spec_re[c * GROUP + t]
            own_im = spec_im[c * GROUP + t]
            cross_re = (own_re * real + own_im * imag).astype(BF16)
            cross_im = (own_re * imag - own_im * real).astype(BF16)
            cross.append(jnp.concatenate([cross_re, cross_im], axis=1))
        half = dot(jnp.concatenate(cross, axis=0), t_back[...]).astype(BF16)
        for t in range(GROUP):
            tile = c * GROUP + t
            block = half[t * length : (t + 1) * length]
            pair = jnp.concatenate([block[:, :length], block[:, length:]], axis=0)
            corr = dot(t_last[...], pair) * (1.0 / float(length * length))
            surfaces[slot, tile] = corr.astype(BF16)
            near = jnp.concatenate([corr[:8], corr[length - 8 :]], axis=0)
            shift_row = offsets[2 * slot, pl.ds(tile, 1)]
            shift_col = offsets[2 * slot + 1, pl.ds(tile, 1)]
            lines = [
                jnp.sum(jnp.where(row_at == shift_row + s, near, 0.0), axis=0, keepdims=True)
                for s in (-1, 0, 1)
            ]
            here = col_at == shift_col
            for s in range(3):
                taps[s, slot, pl.ds(tile, 1)] = jnp.where(here, lines[s], 0.0)
            taps[3, slot, pl.ds(tile, 1)] = jnp.where(col_at == shift_col - 1, lines[1], 0.0)
            taps[4, slot, pl.ds(tile, 1)] = jnp.where(col_at == shift_col + 1, lines[1], 0.0)

    lane_tile = lax.broadcasted_iota(jnp.int32, (tiles, 128), 1)
    row_tile = lax.broadcasted_iota(jnp.int32, (tiles, 128), 0)
    level = floor_ratio * length
    lines = []
    for d in range(REACH):
        value = [jnp.sum(taps[s, d], axis=1, keepdims=True) for s in range(5)]
        for axis, (low, mid, top) in enumerate(((0, 1, 2), (3, 1, 4))):
            low, mid, top = value[low], value[mid], value[top]
            size = jnp.maximum(jnp.abs(low) + jnp.abs(mid) + jnp.abs(top), level)
            found = offsets[2 * d + axis].astype(F32) + (top - low) / size
            for r in range(rows_dev):
                block = found[r * columns : (r + 1) * columns, :columns]
                targets_out[2 * d + axis, r : r + 1, :] = jnp.sum(
                    jnp.where(across == along, block, 0.0), axis=0, keepdims=True
                )
            line = jnp.where(lane_tile == row_tile, found * trust[d], 0.0)
            lines.append(line)
    for k in range(REACH):
        lines[k] = lines[k] + jnp.where(lane_tile == row_tile + tiles, trust[k], 0.0)
    lines = [jnp.sum(line, axis=0, keepdims=True) for line in lines]
    message = jnp.concatenate(lines + [jnp.zeros((8 - 2 * REACH, 128), F32)], axis=0)
    sent_msg[...] = message
    gathered[1, z] = message
    message_from = (sent_msg, sent_msg, sent_msg)
    message_to = (gathered.at[0], gathered.at[1], gathered.at[2])
    fan(message_from, message_to, t_send, t_recv, "start")

    fan_wait(node_from, node_to, n_send, n_recv)
    all_nodes[z] = nodes[...]

    @pl.when(x == 0)
    def _():
        ghosts[0] = jnp.zeros(ghosts.shape[1:], ghosts.dtype)
        gathered[0] = jnp.zeros(gathered.shape[1:], gathered.dtype)

    @pl.when(x == nx - 1)
    def _():
        ghosts[1] = jnp.zeros(ghosts.shape[1:], ghosts.dtype)
        gathered[2] = jnp.zeros(gathered.shape[1:], gathered.dtype)

    @pl.loop(0, nz)
    def _(zz):
        body = all_nodes[zz].astype(F32)
        above = ghosts[0, zz].astype(F32)
        below = ghosts[1, zz].astype(F32)
        for part in range(2):
            vec[0, part, zz + REACH, pl.ds(0, GHOST)] = above[part * GHOST : (part + 1) * GHOST]
            vec[0, part, zz + REACH, pl.ds(GHOST, half_rows)] = body[
                part * half_rows : (part + 1) * half_rows
            ]
            vec[0, part, zz + REACH, pl.ds(GHOST + half_rows, GHOST)] = below[
                part * GHOST : (part + 1) * GHOST
            ]

    fan_wait(message_from, message_to, t_send, t_recv)

    pick_from = lax.broadcasted_iota(jnp.int32, (128, wide), 0)
    pick_to = lax.broadcasted_iota(jnp.int32, (128, wide), 1) // SUB

    def spread(slot, line, base):
        pick = (pick_from == pick_to + (base + line * columns)).astype(F32)
        return jnp.dot(
            gathered[slot].reshape(nz * 8, 128), pick,
            precision=lax.Precision.HIGHEST, preferred_element_type=F32,
        )

    pieces = (
        [(0, rows_dev - 1, 0, GHOST)]
        + [(1, r, GHOST + r * SUB, SUB) for r in range(rows_dev)]
        + [(2, 0, GHOST + half_rows, GHOST)]
    )
    for slot, line, start, count in pieces:
        met[0] = spread(slot, line, 0)
        met[1] = spread(slot, line, rows_dev * columns)

        @pl.loop(0, nz)
        def _(zz):
            for k in range(REACH):
                weight[k, zz + REACH, pl.ds(start, count)] = jnp.broadcast_to(
                    met[1, pl.ds(zz * 8 + k, 1)], (count, wide)
                )
            for part in range(2):
                total = jnp.zeros((1, wide), F32)
                for k in range(REACH):
                    here = met[0, pl.ds(zz * 8 + 2 * k + part, 1)]
                    behind = jnp.maximum(zz - k - 1, 0)
                    back = met[0, pl.ds(behind * 8 + 2 * k + part, 1)]
                    total = total - here + jnp.where(zz > k, back, 0.0)
                vec[ITERS, part, zz + REACH, pl.ds(start, count)] = jnp.broadcast_to(
                    total, (count, wide)
                )

    row_id = lax.broadcasted_iota(jnp.int32, (high, wide), 0)
    col_id = lax.broadcasted_iota(jnp.int32, (high, wide), 1)
    first = jnp.logical_and(row_id == GHOST, x == 0)
    final = jnp.logical_and(row_id == GHOST + half_rows - 1, x == nx - 1)

    def apply(source, target, extra):
        @pl.loop(0, nz)
        def _(zz):
            at = zz + REACH
            for part in range(2):
                v = vec[source, part, at]
                up = jnp.where(first, v, pltpu.roll(v, 1, 0))
                down = jnp.where(final, v, pltpu.roll(v, high - 1, 0))
                left = jnp.where(col_id == 0, v, pltpu.roll(v, 1, 1))
                right = jnp.where(col_id == wide - 1, v, pltpu.roll(v, wide - 1, 1))
                force = lattice_stiff * (up + down + left + right - 4.0 * v)
                if extra is not None:
                    force = force + vec[extra, part, at]
                for k in range(1, REACH + 1):
                    force = force + weight[k - 1, at] * (vec[source, part, at + k] - v)
                    force = force - weight[k - 1, at - k] * (v - vec[source, part, at - k])
                vec[target, part, at] = force

    apply(0, 1, ITERS)
    for i in range(1, ITERS):
        apply(i, i + 1, None)

    pairs = [(i, j) for i in range(ITERS) for j in range(i, ITERS)]

    def products(zz, held):
        held = list(held)
        for part in range(2):
            values = [
                vec[i + 1, part, zz + REACH, pl.ds(GHOST, half_rows)].reshape(
                    half_rows // 8, 8, wide
                )
                for i in range(ITERS)
            ]
            for n, (i, j) in enumerate(pairs):
                held[n] = held[n] + jnp.sum(values[i] * values[j], axis=0)
        return tuple(held)

    held = lax.fori_loop(0, nz, products, tuple(jnp.zeros((8, wide), F32) for _ in pairs))
    lane = lax.broadcasted_iota(jnp.int32, (8, 128), 1)
    gram = jnp.zeros((8, 128), F32)
    for n in range(len(pairs)):
        line = jnp.sum(held[n], axis=0, keepdims=True)
        gram = jnp.where(lane == n, jnp.sum(line, axis=1, keepdims=True), gram)
    mine[...] = gram
    grams[x] = gram

    def gram_copy(xx, where):
        return pltpu.make_async_remote_copy(
            src_ref=mine,
            dst_ref=grams.at[where],
            send_sem=g_send.at[xx],
            recv_sem=g_recv.at[where],
            device_id=(z, xx),
            device_id_type=MESH,
        )

    for xx in range(nx):
        @pl.when(xx != x)
        def _():
            gram_copy(xx, x).start()
    for xx in range(nx):
        @pl.when(xx != x)
        def _():
            gram_copy(xx, xx).wait_recv()
    total = grams[0]
    for xx in range(1, nx):
        total = total + grams[xx]
    total = total[:1]
    lane = lax.broadcasted_iota(jnp.int32, (1, 128), 1)
    inner = {}
    for n, (i, j) in enumerate(pairs):
        inner[i, j] = jnp.sum(jnp.where(lane == n, total, 0.0), axis=1, keepdims=True)
        inner[j, i] = inner[i, j]
    count = 2.0 * nz * nx * half_rows * wide
    factors = [jnp.ones((1, 1), F32)]
    moved = [jnp.zeros((1, 1), F32) for _ in range(ITERS)]
    report = jnp.zeros((1, 128), F32)
    for i in range(ITERS):
        size = jnp.zeros((1, 1), F32)
        for a in range(i + 1):
            for b in range(i + 1):
                size = size + factors[a] * factors[b] * inner[a, b]
        rms = jnp.sqrt(jnp.maximum(size, 0.0) / count + tiny_eps)
        report = jnp.where(lane == i, rms, report)
        step = step_size * jnp.minimum(1.0, clip_level / rms)
        for a in range(i + 1):
            moved[a] = moved[a] + step * factors[a]
        later = factors + [jnp.zeros((1, 1), F32)]
        for a in range(i + 1):
            later[a + 1] = later[a + 1] + step * factors[a]
        factors = later
    rms_out[...] = report[0, :ITERS]
    for part in range(2):
        result = own_nodes[part]
        for i in range(ITERS):
            result = result + moved[i] * vec[i + 1, part, z + REACH, pl.ds(GHOST, half_rows)]
        positions_out[part] = result

    for xx in range(nx):
        @pl.when(xx != x)
        def _():
            gram_copy(xx, x).wait_send()
    fan(node_from, node_to, n_send, n_recv, "wait")
    fan(message_from, message_to, t_send, t_recv, "wait")
    @pl.loop(0, chunks)
    def _(c):
        for kind in range(2):
            @pl.when(own_tests[kind])
            def _():
                own_copy(kind, c).wait_send()
        for slot in range(REACH):
            @pl.when(passes(slot))
            def _():
                passed_copy(slot, c).wait_send()


def deliver(*refs):
    held, out, sems = refs[:4], refs[4:8], refs[8]
    copies = []
    for n in range(4):
        parts = held[n].shape[0] if n == 0 else 1
        for part in range(parts):
            at = pl.ds(part, 1) if n == 0 else slice(None)
            copies.append(
                pltpu.make_async_copy(
                    held[n].at[at] if n == 0 else held[n],
                    out[n].at[at] if n == 0 else out[n],
                    sems.at[len(copies)],
                )
            )
    for copy in copies:
        copy.start()
    for copy in copies:
        copy.wait()


def local(nz, nx, patches, peak_offsets, valid_masks, initial_positions):
    length = patches.shape[-1]
    rows_dev, columns = patches.shape[1:3]
    tiles = rows_dev * columns
    chunks = tiles // GROUP
    half_rows, wide = initial_positions.shape[2:]
    high = half_rows + 2 * GHOST
    own = initial_positions[:, 0]
    grant = min(67043328, (36 << 20) + nz * (nz > 16) * (1 << 20))
    vmem = pl.BlockSpec(memory_space=pltpu.VMEM)
    shapes = (
        jax.ShapeDtypeStruct((REACH, tiles, length, length), BF16),
        jax.ShapeDtypeStruct((2 * REACH, rows_dev, columns), F32),
        jax.ShapeDtypeStruct((2, half_rows, wide), F32),
        jax.ShapeDtypeStruct((ITERS,), F32),
    )
    held = pl.pallas_call(
        functools.partial(kernel, nz, nx, rows_dev, columns),
        out_shape=shapes,
        in_specs=[vmem] * 8,
        out_specs=(vmem,) * 4,
        scratch_shapes=[
            pltpu.VMEM((REACH, tiles, length, length), BF16),
            pltpu.VMEM((tiles, length, length), F32),
            pltpu.VMEM((tiles, length, length), F32),
            pltpu.VMEM((2 * REACH, tiles, 128), jnp.int32),
            pltpu.VMEM((REACH, tiles, 128), F32),
            pltpu.VMEM((2 * half_rows, wide), BF16),
            pltpu.VMEM((2, 2 * GHOST, wide), BF16),
            pltpu.VMEM((5, REACH, tiles, 128), F32),
            pltpu.VMEM((2, nz * 8, wide), F32),
            pltpu.VMEM((8, 128), F32),
            pltpu.VMEM((3, nz, 8, 128), F32),
            pltpu.VMEM((nz, 2 * half_rows, wide), BF16),
            pltpu.VMEM((2, nz, 2 * GHOST, wide), BF16),
            pltpu.VMEM((ITERS + 1, 2, nz + 2 * REACH, high, wide), F32),
            pltpu.VMEM((REACH, nz + REACH, high, wide), F32),
            pltpu.VMEM((nx, 8, 128), F32),
            pltpu.VMEM((8, 128), F32),
            pltpu.SemaphoreType.DMA((REACH + 2, chunks)),
            pltpu.SemaphoreType.DMA((REACH, chunks)),
            pltpu.SemaphoreType.DMA((3, nz)),
            pltpu.SemaphoreType.DMA((3, nz)),
            pltpu.SemaphoreType.DMA((3, nz)),
            pltpu.SemaphoreType.DMA((3, nz)),
            pltpu.SemaphoreType.DMA((nx,)),
            pltpu.SemaphoreType.DMA((nx,)),
        ],
        compiler_params=pltpu.CompilerParams(
            collective_id=0, has_side_effects=True, vmem_limit_bytes=grant
        ),
        name="align",
    )(
        patches.reshape(tiles, length, length), peak_offsets[0], valid_masks[0], own, *tables(length)
    )
    surfaces, targets, positions, rms = pl.pallas_call(
        deliver,
        out_shape=shapes,
        in_specs=[vmem] * 4,
        out_specs=(pl.BlockSpec(memory_space=pl.ANY),) * 4,
        scratch_shapes=[pltpu.SemaphoreType.DMA((REACH + 3,))],
        compiler_params=pltpu.CompilerParams(vmem_limit_bytes=8 << 20),
        name="deliver",
    )(*held)
    return (
        positions[:, None],
        targets[None],
        surfaces.reshape(1, REACH, rows_dev, columns, length, length),
        rms,
    )


def solution(mesh):
    in_specs = (
        P("gz", "xy", None, None, None),
        P("gz", None, "xy", None),
        P("gz", None, "xy", None),
        P(None, "gz", "xy", None),
    )
    out_specs = (
        P(None, "gz", "xy", None),
        P("gz", None, "xy", None),
        P("gz", None, "xy", None, None, None),
        P(),
    )
    body = functools.partial(local, mesh.shape["gz"], mesh.shape["xy"])
    return jax.shard_map(body, mesh=mesh, in_specs=in_specs, out_specs=out_specs, check_vma=False)
```
